256 devices in a mesh: grp: 16 (over z, x_lo), sp: 16 (over x_hi, y, core).
Axes of the slice: x: 4 (x_hi: 2, x_lo: 2; x = x_hi * 2 + x_lo), y: 4, z: 8, core: 2. Of those that a mesh axis runs over, the one named last changes fastest.
Arguments:
- query_rows: bfloat16 [32768, 4096], P(('grp', 'sp')), parts along dimension 0, may hold values from -250 to 250
- key_rows: bfloat16 [32768, 1024], P(('grp', 'sp')), parts along dimension 0, may hold values from -4 to 4
- value_rows: bfloat16 [32768, 1024], P(('grp', 'sp')), parts along dimension 0, may hold values from -6 to 6
- out_grad: bfloat16 [32768, 4096], P(('grp', 'sp')), parts along dimension 0, may hold values from -6 to 6
- question_lengths: int32 [128], P('grp'), parts along dimension 0, may hold values from 1 to 512, 1024 in all
Outputs:
- query_grad: bfloat16 [32768, 4096], P(('grp', 'sp')), parts along dimension 0
- key_grad: bfloat16 [32768, 1024], P(('grp', 'sp')), parts along dimension 0
- value_grad: bfloat16 [32768, 1024], P(('grp', 'sp')), parts along dimension 0
The draws below stay inside these ranges and needn't reach their ends.
There are 16 independent parts, one for each index of `grp`. The reference program is written for one: setup_inputs(seed, part) draws one part's arguments, and reference() takes and returns one part's arrays. A program takes and returns all parts, laid end to end along the dimension named above; each array names one. Nothing has to cross between parts.
All inputs are finite; a program needn't handle non-finite values.
Results may differ from the reference program's by a relative error of at most 0.033.
Values may be sent and summed in bfloat16 or wider, within the bound.
A program may use at most 128 MiB of HBM per device.

```python
import math
import jax
import jax.numpy as jnp
import numpy as np
from jax import lax

HD = 128
QH = 32
KVH = 8
SEQ = 2048
DOC = 1024
QMAX = 512
NQ = 8
BLK = 512


def joint_rows(key):
    folded = jax.random.fold_in(key, 11)
    query_key, keys_key = jax.random.split(folded, 2)
    queries = jnp.clip(jax.random.normal(query_key, (SEQ, QH * HD), jnp.float32), -4.0, 4.0)
    keyset = jnp.clip(jax.random.normal(keys_key, (SEQ, KVH * HD), jnp.float32), -4.0, 4.0)
    return (queries, keyset)


def draw_query_rows(key, part):
    return joint_rows(key)[0].astype(jnp.bfloat16)


def draw_key_rows(key, part):
    return joint_rows(key)[1].astype(jnp.bfloat16)


def steps_of(stream_key, extent, pieces, least, high):
    loudness, own = 1.0, jax.random.fold_in(stream_key, 6)
    for axis_at, shards_of in pieces:
        steps = jnp.exp(jax.random.uniform(jax.random.fold_in(own, axis_at), (shards_of,), jnp.float32, least / len(pieces), high / len(pieces)))
        loudness = loudness * jnp.repeat(steps, extent[axis_at] // shards_of).reshape([-1 if axis == axis_at else 1 for axis in range(len(extent))])
    return loudness


def length_profile(count, total, most, lean):
    weights = [(1 << 20) // math.isqrt(rank ** lean) + 1 for rank in range(2, count + 1)]
    surplus, counts = total - most - (count - 1), [1] * (count - 1)
    while surplus > 0:
        movable = [i for i in range(count - 1) if counts[i] < most]
        whole, left = sum([weights[i] for i in movable]), surplus
        for i in movable:
            more = min(most - counts[i], max(1, left * weights[i] // whole), surplus)
            counts[i] = counts[i] + more
            surplus = surplus - more
    return np.array([most] + counts)


def uneven(rng, count, total, bound, slope):
    if count == 2:
        one = jax.random.randint(rng, (), max(1, total - bound), min(bound, total - 1) + 1)
        return jnp.stack([one, total - one])
    sizes = jnp.asarray(length_profile(count, total, bound, slope), jnp.int32)
    couples = (count - 1) // 2
    giver, taker = sizes[1:1 + 2 * couples:2], sizes[2:2 + 2 * couples:2]
    slack = jnp.minimum(giver - 1, bound - taker)
    shifted = jax.random.randint(jax.random.fold_in(rng, 1), (couples,), 0, 1 << 20) % (slack + 1)
    sizes = sizes.at[1:1 + 2 * couples:2].set(giver - shifted).at[2:2 + 2 * couples:2].set(taker + shifted)
    return sizes[jax.random.permutation(jax.random.fold_in(rng, 2), count)]


def gaussian(rng, extent, spread, bound, cuts=(), held_as=jnp.bfloat16):
    level = steps_of(rng, extent, cuts, -0.22, 0.18) if cuts else 1.0
    values = jax.random.normal(rng, extent, jnp.float32) * spread * level
    return jnp.minimum(jnp.maximum(values, -bound), bound).astype(held_as)


def setup_inputs(seed: int = 0, part: int = 0) -> dict:
    seeds = jax.random.split(jax.random.key(seed), 6)
    part_splits = jax.random.split(jax.random.fold_in(seeds[5], part), 6)
    query_rows = draw_query_rows(jax.random.fold_in(jax.random.fold_in(seeds[5], part), 71), part)
    key_rows = draw_key_rows(jax.random.fold_in(jax.random.fold_in(seeds[5], part), 71), part)
    value_rows = gaussian(part_splits[2], (SEQ, KVH * HD), 1.0, 6.0, ((0, 16),))
    out_grad = gaussian(part_splits[3], (SEQ, QH * HD), 1.0, 6.0, ((0, 16),))
    question_lengths = uneven(part_splits[4], NQ, SEQ - DOC, QMAX, 2).astype(jnp.int32)
    return dict(query_rows=query_rows, key_rows=key_rows, value_rows=value_rows, out_grad=out_grad, question_lengths=question_lengths)


MASKED = -1e+30

def rounded(values):
    return lax.optimization_barrier(values.astype(jnp.bfloat16)).astype(jnp.float32)

def segment_ids(question_lengths):
    ends = jnp.cumsum(question_lengths).astype(jnp.int32)
    places = jnp.arange(SEQ, dtype=jnp.int32)
    inside = lax.optimization_barrier(jnp.sum((ends[None, :] <= (places - DOC)[:, None]).astype(jnp.int32), axis=1))
    return jnp.where(places < DOC, -1, inside).astype(jnp.int32)

def reference(query_rows, key_rows, value_rows, out_grad, question_lengths):
    segment = segment_ids(question_lengths)
    places = jnp.arange(SEQ, dtype=jnp.int32)
    group = QH // KVH
    scaling = 1.0 / math.sqrt(HD)
    block_count = SEQ // BLK
    queries = query_rows.reshape(SEQ, KVH, group, HD).transpose(1, 0, 2, 3)
    grads = out_grad.reshape(SEQ, KVH, group, HD).transpose(1, 0, 2, 3)
    keys = key_rows.reshape(SEQ, KVH, HD).transpose(1, 0, 2)
    values = value_rows.reshape(SEQ, KVH, HD).transpose(1, 0, 2)

    def one_group(packed):
        query_group, grad_group, key_group, value_group = packed
        key_float = key_group.astype(jnp.float32)
        value_float = value_group.astype(jnp.float32)

        def step(carry, block):
            key_sum, value_sum = carry
            start = (block * BLK).astype(jnp.int32)
            query_block = lax.dynamic_slice_in_dim(query_group, start, BLK, 0).astype(jnp.float32)
            grad_block = lax.dynamic_slice_in_dim(grad_group, start, BLK, 0).astype(jnp.float32)
            row_places = lax.dynamic_slice_in_dim(places, start, BLK, 0)
            row_segment = lax.dynamic_slice_in_dim(segment, start, BLK, 0)
            visible = (places[None, :] <= row_places[:, None]) & ((places[None, :] < DOC) | (segment[None, :] == row_segment[:, None]))
            scores = jnp.einsum('bgd,sd->gbs', query_block, key_float) * scaling
            scores = jnp.where(visible[None], scores, MASKED)
            peak = lax.optimization_barrier(jnp.max(scores, axis=2))
            log_total = peak + jnp.log(lax.optimization_barrier(jnp.sum(jnp.exp(scores - peak[..., None]), axis=2)))
            probs = jnp.exp(scores - log_total[..., None])
            probs_b = rounded(probs)
            output = rounded(jnp.einsum('gbs,sd->bgd', probs_b, value_float))
            delta = lax.optimization_barrier(jnp.sum(grad_block * output, axis=2)).T
            value_sum = value_sum + jnp.einsum('gbs,bgd->sd', probs_b, grad_block)
            prob_grad = jnp.einsum('bgd,sd->gbs', grad_block, value_float)
            score_grad = rounded(probs * (prob_grad - delta[..., None]))
            query_part = (jnp.einsum('gbs,sd->bgd', score_grad, key_float) * scaling).astype(jnp.bfloat16)
            key_sum = key_sum + jnp.einsum('gbs,bgd->sd', score_grad, query_block) * scaling
            return ((key_sum, value_sum), query_part)
        empty = jnp.zeros((SEQ, HD), jnp.float32)
        sums, query_parts = lax.scan(step, (empty, empty), jnp.arange(block_count, dtype=jnp.int32))
        return (query_parts.reshape(SEQ, group, HD), sums[0].astype(jnp.bfloat16), sums[1].astype(jnp.bfloat16))
    query_all, key_all, value_all = lax.map(one_group, (queries, grads, keys, values))
    query_grad = query_all.transpose(1, 0, 2, 3).reshape(SEQ, QH * HD)
    key_grad = key_all.transpose(1, 0, 2).reshape(SEQ, KVH * HD)
    value_grad = value_all.transpose(1, 0, 2).reshape(SEQ, KVH * HD)
    return (query_grad, key_grad, value_grad)
```

```python
import functools
import math

import jax
import jax.numpy as jnp
from jax import lax
from jax.experimental import pallas as pl
from jax.experimental.pallas import tpu as pltpu
from jax.sharding import PartitionSpec as P

HD = 128
QH = 32
KVH = 8
SEQ = 2048
DOC = 1024
NQ = 8
TOK = 128
BLK = 256
DEVS = 16
MASKED = -1e30
MESH = pl.DeviceIdType.MESH
BF = jnp.bfloat16
F32 = jnp.float32

PARTNERS = tuple(
    (a, b, c)
    for c in (0, 1)
    for a, b in ((1, 2), (1, 1), (0, 2), (1, 3), (1, 0), (0, 1), (0, 3), (0, 0))
    if (a, b, c) != (0, 0, 0)
)


def dot_t(a, b):
    return lax.dot_general(a, b, (((1,), (1,)), ((), ())), preferred_element_type=F32)


def dot_n(a, b):
    return lax.dot_general(a, b, (((1,), (0,)), ((), ())), preferred_element_type=F32)


def fold(x, op):
    return op(x.reshape(x.shape[0] // 8, 8, x.shape[1]), axis=0)


def kernel(
    lens,
    q_hbm,
    k_hbm,
    v_hbm,
    do_hbm,
    dq_out,
    dk_out,
    dv_out,
    qb,
    dob,
    kb,
    vb,
    kt,
    s_buf,
    dp_buf,
    dka,
    dva,
    dqb,
    part,
    fin,
    send_kv,
    recv_kv,
    send_q,
    recv_q,
    relay_kv,
    send_dq,
    recv_dq,
    send_part,
    recv_part,
    send_fin,
    recv_fin,
):
    grp = lax.axis_index("grp")
    me = lax.axis_index("sp")
    far = me // 8
    yy = (me // 2) % 4
    core = me % 2
    chip = me // 2
    other = chip * 2 + 1 - core
    scaling = 1.0 / math.sqrt(HD)
    to_log2 = scaling * math.log2(math.e)

    def partner(step):
        a, b, c = step
        return ((far + a) % 2) * 8 + ((yy + b) % 4) * 2 + (core + c) % 2

    def lanes(index, width=HD):
        return pl.ds(pl.multiple_of(index * width, width), width)

    def rows(index, width=TOK):
        return pl.ds(pl.multiple_of(index * width, width), width)

    def remote(src, dst, ss, rs, dev):
        return pltpu.make_async_remote_copy(
            src_ref=src, dst_ref=dst, send_sem=ss, recv_sem=rs, device_id=(grp, dev), device_id_type=MESH
        )

    barrier = pltpu.get_barrier_semaphore()
    for step in PARTNERS:
        pl.semaphore_signal(barrier, inc=1, device_id=(grp, partner(step)), device_id_type=MESH)
    pl.semaphore_wait(barrier, len(PARTNERS))

    kv = ((k_hbm, kb), (v_hbm, vb))
    qd = ((q_hbm, qb), (do_hbm, dob))

    for step in PARTNERS:
        if step[2] == 0:
            dev = partner(step)
            for t, (src, dst) in enumerate(kv):
                remote(
                    src.at[:, lanes(dev // 2)], dst.at[rows(me)], send_kv.at[t, dev], recv_kv.at[t, me], dev
                ).start()
    for t, (src, dst) in enumerate(kv):
        pltpu.make_async_copy(src.at[:, lanes(chip)], dst.at[rows(me)], recv_kv.at[t, me]).start()
        remote(
            src.at[:, lanes(chip)], dst.at[rows(me)], relay_kv.at[t, me], recv_kv.at[t, me], other
        ).start()
    for h in (0, 1):
        for step in PARTNERS:
            dev = partner(step)
            for t, (src, dst) in enumerate(qd):
                remote(
                    src.at[:, lanes(dev * 2 + h)],
                    dst.at[h, rows(me)],
                    send_q.at[t, h, dev],
                    recv_q.at[t, h, me],
                    dev,
                ).start()
        for t, (src, dst) in enumerate(qd):
            pltpu.make_async_copy(src.at[:, lanes(me * 2 + h)], dst.at[h, rows(me)], recv_q.at[t, h, me]).start()

    dka[...] = jnp.zeros_like(dka)
    dva[...] = jnp.zeros_like(dva)

    def landed(t, dev):
        dst = kv[t][1]
        remote(dst.at[rows(dev)], dst.at[rows(dev)], relay_kv.at[t, dev], recv_kv.at[t, dev], other).wait_recv()

    def take(dev):
        kt[:, lanes(dev)] = kb[rows(dev), :].T

    def relay(i, carry):
        dev = ((chip + 7 - i) % 8) * 2 + core
        for t in (0, 1):
            landed(t, dev)

        @pl.when(dev != me)
        def _():
            for t in (0, 1):
                dst = kv[t][1]
                remote(
                    dst.at[rows(dev)], dst.at[rows(dev)], relay_kv.at[t, dev], recv_kv.at[t, dev], other
                ).start()

        take(dev)
        return carry

    lax.fori_loop(0, 8, relay, 0)

    def from_other(i, carry):
        dev = ((chip + 7 - i) % 8) * 2 + 1 - core
        for t in (0, 1):
            landed(t, dev)
        take(dev)
        return carry

    lax.fori_loop(0, 8, from_other, 0)

    def attend(h, rb, chunks, question):
        here = rows(rb, BLK)
        for dev in (rb * 2, rb * 2 + 1):
            for t in (0, 1):
                dst = qd[t][1]
                remote(
                    dst.at[h, rows(dev)], dst.at[h, rows(dev)], send_q.at[t, h, dev], recv_q.at[t, h, dev], other
                ).wait_recv()
        query = qb[h, here, :]
        grad = dob[h, here, :]
        i_pos = rb * BLK + lax.broadcasted_iota(jnp.int32, (1, BLK), 1)
        first = jnp.zeros((1, BLK), jnp.int32)
        if question:
            end = jnp.int32(DOC)
            first = first + DOC
            for c in range(NQ - 1):
                end = end + lens[c]
                first = jnp.where(i_pos >= end, end, first)
        peak = None
        for t, (chunk, masked) in enumerate(chunks):
            keys = rows(chunk, BLK)
            score = dot_t(kb[keys, :], query)
            if masked:
                j_pos = chunk * BLK + lax.broadcasted_iota(jnp.int32, (BLK, BLK), 0)
                seen = j_pos <= i_pos
                if question:
                    seen = seen & (j_pos >= first)
                score = jnp.where(seen, score, MASKED)
            s_buf[pl.ds(t * BLK, BLK), :] = score
            dp_buf[pl.ds(t * BLK, BLK), :] = dot_t(vb[keys, :], grad)
            top = fold(score, jnp.max)
            peak = top if peak is None else jnp.maximum(peak, top)
        peak = jnp.max(peak, axis=0, keepdims=True)
        total = jnp.zeros((8, BLK), F32)
        weighted = jnp.zeros((8, BLK), F32)
        for t in range(len(chunks)):
            at = pl.ds(t * BLK, BLK)
            prob = jnp.exp2((s_buf[at, :] - peak) * to_log2)
            s_buf[at, :] = prob
            total = total + fold(prob, jnp.sum)
            weighted = weighted + fold(prob * dp_buf[at, :], jnp.sum)
        inverse = 1.0 / jnp.sum(total, axis=0, keepdims=True)
        delta = jnp.sum(weighted, axis=0, keepdims=True) * inverse
        dq_t = jnp.zeros((HD, BLK), F32)
        for t, (chunk, _) in enumerate(chunks):
            at = pl.ds(t * BLK, BLK)
            keys = rows(chunk, BLK)
            prob = s_buf[at, :] * inverse
            score_grad = (prob * (dp_buf[at, :] - delta)).astype(BF)
            dva[keys, :] += dot_n(prob.astype(BF), grad)
            dka[keys, :] += dot_n(score_grad, query)
            dq_t = dq_t + dot_n(kt[:, lanes(chunk, BLK)], score_grad)
        dqb[h, here, :] = (dq_t * scaling).T.astype(BF)
        for dev in (rb * 2, rb * 2 + 1):
            src = dqb.at[h, rows(dev)]
            dst = dq_out.at[:, lanes(me * 2 + h)]

            @pl.when(dev == me)
            def _(src=src, dst=dst):
                pltpu.make_async_copy(src, dst, recv_dq.at[h, me]).start()

            @pl.when(dev != me)
            def _(src=src, dst=dst, dev=dev):
                remote(src, dst, send_dq.at[h, dev], recv_dq.at[h, me], dev).start()

    acc = (dka, dva)
    outs = (dk_out, dv_out)

    def part_copy(t, rb):
        return remote(
            acc[t].at[rows(rb * 2 + 1 - core)], part.at[rb, t], send_part.at[t, rb], recv_part.at[t, rb], other
        )

    def finish(rb):
        dev = rb * 2 + core
        for t in (0, 1):
            part_copy(t, rb).wait_recv()
            both = acc[t][rows(dev), :] + part[rb, t]
            if t == 0:
                both = both * scaling
            fin[rb, t] = both.astype(BF)
        for t in (0, 1):
            src = fin.at[rb, t]
            dst = outs[t].at[:, lanes(chip)]

            @pl.when(dev == me)
            def _(src=src, dst=dst, t=t):
                pltpu.make_async_copy(src, dst, recv_fin.at[t, chip]).start()

            @pl.when(dev != me)
            def _(src=src, dst=dst, t=t):
                remote(src, dst, send_fin.at[t, rb], recv_fin.at[t, chip], dev).start()

    def head(h, carry):
        def question_rows(i, c):
            rb = 7 - i
            chunks = [(n, False) for n in range(4)] + [(rb - 2 + n, True) for n in range(3)]
            attend(h, rb, chunks, True)

            @pl.when(h == 1)
            def _():
                for t in (0, 1):
                    part_copy(t, rb).start()

                @pl.when(i > 0)
                def _():
                    finish(rb + 1)

            return c

        lax.fori_loop(0, 4, question_rows, 0)
        for rb in (3, 2, 1, 0):
            attend(h, rb, [(n, n == rb) for n in range(rb + 1)], False)

            @pl.when(h == 1)
            def _(rb=rb):
                for t in (0, 1):
                    part_copy(t, rb).start()
                finish(rb + 1)

        return carry

    lax.fori_loop(0, 2, head, 0)
    finish(0)

    for step in PARTNERS:
        dev = partner(step)
        for t, (src, dst) in enumerate(qd):
            for h in (0, 1):
                remote(
                    src.at[:, lanes(dev * 2 + h)], dst.at[h, rows(me)], send_q.at[t, h, dev], recv_q.at[t, h, me], dev
                ).wait_send()
        for h in (0, 1):
            remote(
                dqb.at[h, rows(dev)], dq_out.at[:, lanes(dev * 2 + h)], send_dq.at[h, dev], recv_dq.at[h, dev], dev
            ).wait()
        if step[2] == 0:
            for t, (src, dst) in enumerate(kv):
                remote(
                    src.at[:, lanes(dev // 2)], dst.at[rows(me)], send_kv.at[t, dev], recv_kv.at[t, me], dev
                ).wait_send()
                remote(
                    dst.at[rows(dev)], dst.at[rows(dev)], relay_kv.at[t, dev], recv_kv.at[t, dev], other
                ).wait_send()
                remote(
                    fin.at[dev // 2, t],
                    outs[t].at[:, lanes(dev // 2)],
                    send_fin.at[t, dev // 2],
                    recv_fin.at[t, dev // 2],
                    dev,
                ).wait()
    for h in (0, 1):
        pltpu.make_async_copy(
            dqb.at[h, rows(me)], dq_out.at[:, lanes(me * 2 + h)], recv_dq.at[h, me]
        ).wait()
    for t, (src, dst) in enumerate(kv):
        remote(
            src.at[:, lanes(chip)], dst.at[rows(me)], relay_kv.at[t, me], recv_kv.at[t, me], other
        ).wait_send()
        pltpu.make_async_copy(fin.at[chip, t], outs[t].at[:, lanes(chip)], recv_fin.at[t, chip]).wait()
        for rb in range(8):
            part_copy(t, rb).wait_send()


def on_device(query_rows, key_rows, value_rows, out_grad, question_lengths):
    any_space = pl.BlockSpec(memory_space=pl.ANY)
    dma = pltpu.SemaphoreType.DMA
    return pl.pallas_call(
        kernel,
        name="exchange_attend",
        out_shape=(
            jax.ShapeDtypeStruct((TOK, QH * HD), BF),
            jax.ShapeDtypeStruct((TOK, KVH * HD), BF),
            jax.ShapeDtypeStruct((TOK, KVH * HD), BF),
        ),
        in_specs=[pl.BlockSpec(memory_space=pltpu.SMEM)] + [any_space] * 4,
        out_specs=(any_space,) * 3,
        scratch_shapes=[
            pltpu.VMEM((2, SEQ, HD), BF),
            pltpu.VMEM((2, SEQ, HD), BF),
            pltpu.VMEM((SEQ, HD), BF),
            pltpu.VMEM((SEQ, HD), BF),
            pltpu.VMEM((HD, SEQ), BF),
            pltpu.VMEM((7 * BLK, BLK), F32),
            pltpu.VMEM((7 * BLK, BLK), F32),
            pltpu.VMEM((SEQ, HD), F32),
            pltpu.VMEM((SEQ, HD), F32),
            pltpu.VMEM((2, SEQ, HD), BF),
            pltpu.VMEM((8, 2, TOK, HD), F32),
            pltpu.VMEM((8, 2, TOK, HD), BF),
            dma((2, DEVS)),
            dma((2, DEVS)),
            dma((2, 2, DEVS)),
            dma((2, 2, DEVS)),
            dma((2, DEVS)),
            dma((2, DEVS)),
            dma((2, DEVS)),
            dma((2, 8)),
            dma((2, 8)),
            dma((2, 8)),
            dma((2, 8)),
        ],
        compiler_params=pltpu.CompilerParams(
            collective_id=0, has_side_effects=True, vmem_limit_bytes=48 * 1024 * 1024
        ),
    )(question_lengths, query_rows, key_rows, value_rows, out_grad)


def solution(mesh):
    spec = P(("grp", "sp"), None)
    return jax.shard_map(
        on_device,
        mesh=mesh,
        in_specs=(spec, spec, spec, spec, P("grp")),
        out_specs=(spec, spec, spec),
        check_vma=False,
    )
```

```python
import functools
import math

import jax
import jax.numpy as jnp
from jax import lax
from jax.experimental import pallas as pl
from jax.experimental.pallas import tpu as pltpu
from jax.sharding import PartitionSpec as P

HD = 128
QH = 32
KVH = 8
SEQ = 2048
DOC = 1024
NQ = 8
TOK = 128
HALF = 64
BLK = 256
DEVS = 16
MASKED = -1e30
MESH = pl.DeviceIdType.MESH
BF = jnp.bfloat16
F32 = jnp.float32

PARTNERS = tuple(
    (a, b, c)
    for c in (0, 1)
    for a, b in ((1, 2), (1, 1), (0, 2), (1, 3), (1, 0), (0, 1), (0, 3), (0, 0))
    if (a, b, c) != (0, 0, 0)
)


def dot_t(a, b):
    return lax.dot_general(a, b, (((1,), (1,)), ((), ())), preferred_element_type=F32)


def dot_n(a, b):
    return lax.dot_general(a, b, (((1,), (0,)), ((), ())), preferred_element_type=F32)


def fold(x, op):
    return op(x.reshape(x.shape[0] // 8, 8, x.shape[1]), axis=0)


def kernel(
    lens,
    q_hbm,
    k_hbm,
    v_hbm,
    do_hbm,
    dq_out,
    dk_out,
    dv_out,
    qd,
    kb,
    vb,
    kt,
    s_buf,
    dp_buf,
    dka,
    dva,
    dqb,
    part,
    fin,
    send_kv,
    recv_kv,
    relay_kv,
    send_q,
    recv_q,
    send_dq,
    recv_dq,
    send_part,
    recv_part,
    send_fin,
    recv_fin,
):
    grp = lax.axis_index("grp")
    me = lax.axis_index("sp")
    far = me // 8
    yy = (me // 2) % 4
    core = me % 2
    chip = me // 2
    other = chip * 2 + 1 - core
    scaling = 1.0 / math.sqrt(HD)
    to_log2 = scaling * math.log2(math.e)

    def partner(step):
        a, b, c = step
        return ((far + a) % 2) * 8 + ((yy + b) % 4) * 2 + (core + c) % 2

    def lanes(index, width=HD):
        return pl.ds(pl.multiple_of(index * width, width), width)

    def rows(index, width=TOK):
        return pl.ds(pl.multiple_of(index * width, width), width)

    def remote(src, dst, ss, rs, dev):
        return pltpu.make_async_remote_copy(
            src_ref=src, dst_ref=dst, send_sem=ss, recv_sem=rs, device_id=(grp, dev), device_id_type=MESH
        )

    def local(src, dst, sem):
        return pltpu.make_async_copy(src, dst, sem)

    barrier = pltpu.get_barrier_semaphore()
    for step in PARTNERS:
        pl.semaphore_signal(barrier, inc=1, device_id=(grp, partner(step)), device_id_type=MESH)
    pl.semaphore_wait(barrier, len(PARTNERS))

    kv = ((k_hbm, kb), (v_hbm, vb))
    qs = (q_hbm, do_hbm)

    for step in PARTNERS:
        if step[2] == 0:
            dev = partner(step)
            for t, (src, dst) in enumerate(kv):
                remote(src.at[:, lanes(dev // 2)], dst.at[rows(me)], send_kv.at[t], recv_kv.at[t, me], dev).start()
    for t, (src, dst) in enumerate(kv):
        local(src.at[:, lanes(chip)], dst.at[rows(me)], recv_kv.at[t, me]).start()
        remote(src.at[:, lanes(chip)], dst.at[rows(me)], relay_kv.at[t], recv_kv.at[t, me], other).start()
    for h in (0, 1):
        for half in (0, 1):
            top = pl.ds(half * HALF, HALF)
            for step in PARTNERS:
                dev = partner(step)
                for t, src in enumerate(qs):
                    remote(
                        src.at[top, lanes(dev * 2 + h)],
                        qd.at[h, half, me, t],
                        send_q.at[t],
                        recv_q.at[h, half, me // 4],
                        dev,
                    ).start()
            for t, src in enumerate(qs):
                local(src.at[top, lanes(me * 2 + h)], qd.at[h, half, me, t], recv_q.at[h, half, me // 4]).start()

    dka[...] = jnp.zeros_like(dka)
    dva[...] = jnp.zeros_like(dva)

    def take(dev, pass_on):
        for t, (_, dst) in enumerate(kv):
            remote(dst.at[rows(dev)], dst.at[rows(dev)], relay_kv.at[t], recv_kv.at[t, dev], other).wait_recv()
        if pass_on:

            @pl.when(dev != me)
            def _():
                for t, (_, dst) in enumerate(kv):
                    remote(dst.at[rows(dev)], dst.at[rows(dev)], relay_kv.at[t], recv_kv.at[t, dev], other).start()

        kt[:, lanes(dev)] = kb[rows(dev), :].T

    def from_far(i, carry):
        take(((chip + 7 - i) % 8) * 2 + core, True)
        return carry

    def from_other(i, carry):
        take(((chip + 7 - i) % 8) * 2 + 1 - core, False)
        return carry

    lax.fori_loop(0, 8, from_far, 0)
    lax.fori_loop(0, 8, from_other, 0)

    def attend(h, half, span, chunks, question):
        four = pl.ds(span * 4, 4)
        local(qd.at[h, half, four], qd.at[h, half, four], recv_q.at[h, half, span]).wait()
        query = qd[h, half, four, 0].reshape(BLK, HD)
        grad = qd[h, half, four, 1].reshape(BLK, HD)
        lane = lax.broadcasted_iota(jnp.int32, (1, BLK), 1)
        i_pos = span * (4 * TOK) + half * HALF + lane + (lane >> 6) * (TOK - HALF)
        first = jnp.zeros((1, BLK), jnp.int32)
        if question:
            end = jnp.int32(DOC)
            first = first + DOC
            for c in range(NQ - 1):
                end = end + lens[c]
                first = jnp.where(i_pos >= end, end, first)
        peak = None
        for t, (chunk, masked) in enumerate(chunks):
            keys = rows(chunk, BLK)
            score = dot_t(kb[keys, :], query)
            if masked:
                j_pos = chunk * BLK + lax.broadcasted_iota(jnp.int32, (BLK, BLK), 0)
                seen = j_pos <= i_pos
                if question:
                    seen = seen & (j_pos >= first)
                score = jnp.where(seen, score, MASKED)
            s_buf[pl.ds(t * BLK, BLK), :] = score
            dp_buf[pl.ds(t * BLK, BLK), :] = dot_t(vb[keys, :], grad)
            top = fold(score, jnp.max)
            peak = top if peak is None else jnp.maximum(peak, top)
        peak = jnp.max(peak, axis=0, keepdims=True)
        total = jnp.zeros((8, BLK), F32)
        weighted = jnp.zeros((8, BLK), F32)
        for t in range(len(chunks)):
            at = pl.ds(t * BLK, BLK)
            prob = jnp.exp2((s_buf[at, :] - peak) * to_log2)
            s_buf[at, :] = prob
            total = total + fold(prob, jnp.sum)
            weighted = weighted + fold(prob * dp_buf[at, :], jnp.sum)
        inverse = 1.0 / jnp.sum(total, axis=0, keepdims=True)
        delta = jnp.sum(weighted, axis=0, keepdims=True) * inverse
        dq_t = jnp.zeros((HD, BLK), F32)
        for t, (chunk, _) in enumerate(chunks):
            at = pl.ds(t * BLK, BLK)
            keys = rows(chunk, BLK)
            prob = s_buf[at, :] * inverse
            score_grad = (prob * (dp_buf[at, :] - delta)).astype(BF)
            dva[keys, :] += dot_n(prob.astype(BF), grad)
            dka[keys, :] += dot_n(score_grad, query)
            dq_t = dq_t + dot_n(kt[:, lanes(chunk, BLK)], score_grad)
        dqb[four, h, half] = (dq_t * scaling).T.astype(BF).reshape(4, HALF, HD)

        def give(n, carry):
            dev = span * 4 + n
            src = dqb.at[dev, h, half]
            dst = dq_out.at[pl.ds(pl.multiple_of(half * HALF, HALF), HALF), lanes(me * 2 + h)]

            @pl.when(dev == me)
            def _():
                local(src, dst, recv_dq).start()

            @pl.when(dev != me)
            def _():
                remote(src, dst, send_dq, recv_dq, dev).start()

            return carry

        lax.fori_loop(0, 4, give, 0)

    acc = (dka, dva)
    outs = (dk_out, dv_out)

    def share(rb):
        for t in (0, 1):
            remote(acc[t].at[rows(rb * 2 + 1 - core)], part.at[rb, t], send_part, recv_part.at[rb], other).start()

    def close(rb):
        dev = rb * 2 + core
        local(part.at[rb], part.at[rb], recv_part.at[rb]).wait()
        for t in (0, 1):
            both = acc[t][rows(dev), :] + part[rb, t]
            if t == 0:
                both = both * scaling
            fin[rb, t] = both.astype(BF)
        for t in (0, 1):
            src = fin.at[rb, t]
            dst = outs[t].at[:, lanes(chip)]

            @pl.when(dev == me)
            def _(src=src, dst=dst, t=t):
                local(src, dst, recv_fin.at[t]).start()

            @pl.when(dev != me)
            def _(src=src, dst=dst, t=t):
                remote(src, dst, send_fin, recv_fin.at[t], dev).start()

    def chunk_step(n, carry):
        h = n // 2
        half = n % 2
        last = n // 3

        def span_step(i, c):
            span = last * (3 - i) + (1 - last) * ((chip // 2 + 1 + i) % 4)

            @pl.when(span >= 2)
            def _():
                chunks = [(m, False) for m in range(4)] + [(span * 2 - 2 + m, True) for m in range(4)]
                attend(h, half, span, chunks, True)

            for doc in (0, 1):

                @pl.when(span == doc)
                def _(doc=doc):
                    attend(h, half, doc, [(m, m >= doc * 2) for m in range(doc * 2 + 2)], False)

            @pl.when(last == 1)
            def _():
                share(span * 2)
                share(span * 2 + 1)

                @pl.when(i > 0)
                def _():
                    close(span * 2 + 2)
                    close(span * 2 + 3)

            return c

        lax.fori_loop(0, 4, span_step, 0)
        return carry

    lax.fori_loop(0, 4, chunk_step, 0)
    close(0)
    close(1)

    for t, (src, _) in enumerate(kv):
        local(src.at[:, pl.ds(0, 7 * HD)], src.at[:, pl.ds(0, 7 * HD)], send_kv.at[t]).wait()
        local(src, src, relay_kv.at[t]).wait()
    for t, src in enumerate(qs):
        local(src.at[:, pl.ds(0, 30 * HD)], src.at[:, pl.ds(0, 30 * HD)], send_q.at[t]).wait()
    local(part, part, send_part).wait()
    local(dqb.at[pl.ds(0, 15)], dqb.at[pl.ds(0, 15)], send_dq).wait()
    local(fin.at[pl.ds(0, 7)], fin.at[pl.ds(0, 7)], send_fin).wait()
    local(dq_out, dq_out, recv_dq).wait()
    for t in (0, 1):
        local(outs[t], outs[t], recv_fin.at[t]).wait()


def put(dq, dk, dv, dq_out, dk_out, dv_out, sems):
    copies = [
        pltpu.make_async_copy(src, dst, sems.at[n])
        for n, (src, dst) in enumerate(((dq, dq_out), (dk, dk_out), (dv, dv_out)))
    ]
    for copy in copies:
        copy.start()
    for copy in copies:
        copy.wait()


def on_device(query_rows, key_rows, value_rows, out_grad, question_lengths):
    hbm = pl.BlockSpec(memory_space=pltpu.HBM)
    any_space = pl.BlockSpec(memory_space=pl.ANY)
    dma = pltpu.SemaphoreType.DMA
    grads = pl.pallas_call(
        kernel,
        name="exchange_attend",
        out_shape=(
            pltpu.VMEM((TOK, QH * HD), BF),
            pltpu.VMEM((TOK, KVH * HD), BF),
            pltpu.VMEM((TOK, KVH * HD), BF),
        ),
        in_specs=[pl.BlockSpec(memory_space=pltpu.SMEM)] + [hbm] * 4,
        out_specs=(any_space,) * 3,
        scratch_shapes=[
            pltpu.VMEM((2, 2, DEVS, 2, HALF, HD), BF),
            pltpu.VMEM((SEQ, HD), BF),
            pltpu.VMEM((SEQ, HD), BF),
            pltpu.VMEM((HD, SEQ), BF),
            pltpu.VMEM((8 * BLK, BLK), F32),
            pltpu.VMEM((8 * BLK, BLK), F32),
            pltpu.VMEM((SEQ, HD), F32),
            pltpu.VMEM((SEQ, HD), F32),
            pltpu.VMEM((DEVS, 2, 2, HALF, HD), BF),
            pltpu.VMEM((8, 2, TOK, HD), F32),
            pltpu.VMEM((8, 2, TOK, HD), BF),
            dma((2,)),
            dma((2, DEVS)),
            dma((2,)),
            dma((2,)),
            dma((2, 2, 4)),
            dma,
            dma,
            dma,
            dma((8,)),
            dma,
            dma((2,)),
        ],
        compiler_params=pltpu.CompilerParams(
            collective_id=0, has_side_effects=True, vmem_limit_bytes=60 * 1024 * 1024
        ),
    )(question_lengths, query_rows, key_rows, value_rows, out_grad)
    return pl.pallas_call(
        put,
        name="put",
        out_shape=(
            jax.ShapeDtypeStruct((TOK, QH * HD), BF),
            jax.ShapeDtypeStruct((TOK, KVH * HD), BF),
            jax.ShapeDtypeStruct((TOK, KVH * HD), BF),
        ),
        in_specs=[any_space] * 3,
        out_specs=(any_space,) * 3,
        scratch_shapes=[dma((3,))],
    )(*(pltpu.with_memory_space_constraint(g, pltpu.VMEM) for g in grads))


def solution(mesh):
    spec = P(("grp", "sp"), None)
    return jax.shard_map(
        on_device,
        mesh=mesh,
        in_specs=(spec, spec, spec, spec, P("grp")),
        out_specs=(spec, spec, spec),
        check_vma=False,
    )
```

```python
import functools
import math

import jax
import jax.numpy as jnp
from jax import lax
from jax.experimental import pallas as pl
from jax.experimental.pallas import tpu as pltpu
from jax.sharding import PartitionSpec as P

HD = 128
QH = 32
KVH = 8
SEQ = 2048
DOC = 1024
NQ = 8
TOK = 128
HALF = 64
BLK = 256
DEVS = 16
STRIP = 64
MASKED = -1e30
MESH = pl.DeviceIdType.MESH
BF = jnp.bfloat16
F32 = jnp.float32

PARTNERS = tuple(
    (a, b, c)
    for c in (0, 1)
    for a, b in ((1, 2), (1, 1), (0, 2), (1, 3), (1, 0), (0, 1), (0, 3), (0, 0))
    if (a, b, c) != (0, 0, 0)
)


def dot_t(a, b):
    return lax.dot_general(a, b, (((1,), (1,)), ((), ())), preferred_element_type=F32)


def dot_n(a, b):
    return lax.dot_general(a, b, (((1,), (0,)), ((), ())), preferred_element_type=F32)


def fold(x, op):
    return op(x.reshape(x.shape[0] // 8, 8, x.shape[1]), axis=0)


def kernel(
    lens,
    q_hbm,
    k_hbm,
    v_hbm,
    do_hbm,
    dq_out,
    dk_out,
    dv_out,
    qd,
    kb,
    vb,
    kt,
    s_buf,
    dp_buf,
    dka,
    dva,
    dqb,
    part,
    fin,
    send_kv,
    recv_kv,
    relay_kv,
    send_q,
    recv_q,
    send_dq,
    recv_dq,
    send_part,
    recv_part,
    send_fin,
    recv_fin,
):
    grp = lax.axis_index("grp")
    me = lax.axis_index("sp")
    far = me // 8
    yy = (me // 2) % 4
    core = me % 2
    chip = me // 2
    other = chip * 2 + 1 - core
    scaling = 1.0 / math.sqrt(HD)
    to_log2 = scaling * math.log2(math.e)

    def partner(step):
        a, b, c = step
        return ((far + a) % 2) * 8 + ((yy + b) % 4) * 2 + (core + c) % 2

    def lanes(index, width=HD):
        return pl.ds(pl.multiple_of(index * width, width), width)

    def rows(index, width=TOK):
        return pl.ds(pl.multiple_of(index * width, width), width)

    def remote(src, dst, ss, rs, dev):
        return pltpu.make_async_remote_copy(
            src_ref=src, dst_ref=dst, send_sem=ss, recv_sem=rs, device_id=(grp, dev), device_id_type=MESH
        )

    def local(src, dst, sem):
        return pltpu.make_async_copy(src, dst, sem)

    barrier = pltpu.get_barrier_semaphore()
    for step in PARTNERS:
        pl.semaphore_signal(barrier, inc=1, device_id=(grp, partner(step)), device_id_type=MESH)
    dka[...] = jnp.zeros_like(dka)
    dva[...] = jnp.zeros_like(dva)
    pl.semaphore_wait(barrier, len(PARTNERS))

    kv = ((k_hbm, kb), (v_hbm, vb))
    qs = (q_hbm, do_hbm)

    for step in PARTNERS:
        if step[2] == 0:
            dev = partner(step)
            for t, (src, dst) in enumerate(kv):
                remote(src.at[:, lanes(dev // 2)], dst.at[rows(me)], send_kv.at[t], recv_kv.at[t, me], dev).start()
    for t, (src, dst) in enumerate(kv):
        local(src.at[:, lanes(chip)], dst.at[rows(me)], recv_kv.at[t, me]).start()
        remote(src.at[:, lanes(chip)], dst.at[rows(me)], relay_kv.at[t], recv_kv.at[t, me], other).start()
    for h in (0, 1):
        for half in (0, 1):
            top = pl.ds(half * HALF, HALF)
            for step in PARTNERS:
                dev = partner(step)
                for t, src in enumerate(qs):
                    remote(
                        src.at[top, lanes(dev * 2 + h)],
                        qd.at[h, half, me, t],
                        send_q.at[t],
                        recv_q.at[h, half, me // 4],
                        dev,
                    ).start()
            for t, src in enumerate(qs):
                local(src.at[top, lanes(me * 2 + h)], qd.at[h, half, me, t], recv_q.at[h, half, me // 4]).start()

    def take(dev, pass_on):
        for t, (_, dst) in enumerate(kv):
            remote(dst.at[rows(dev)], dst.at[rows(dev)], relay_kv.at[t], recv_kv.at[t, dev], other).wait_recv()
        if pass_on:

            @pl.when(dev != me)
            def _():
                for t, (_, dst) in enumerate(kv):
                    remote(dst.at[rows(dev)], dst.at[rows(dev)], relay_kv.at[t], recv_kv.at[t, dev], other).start()

        kt[:, lanes(dev)] = kb[rows(dev), :].T

    def from_far(i, carry):
        take(((chip + 7 - i) % 8) * 2 + core, True)
        return carry

    def from_other(i, carry):
        take(((chip + 7 - i) % 8) * 2 + 1 - core, False)
        return carry

    lax.fori_loop(0, 8, from_far, 0)
    lax.fori_loop(0, 8, from_other, 0)

    def load(h, half, span, slot):
        four = pl.ds(span * 4, 4)
        local(qd.at[h, half, four], qd.at[h, half, four], recv_q.at[h, half, span]).wait()
        question = span >= 2
        lane = lax.broadcasted_iota(jnp.int32, (1, BLK), 1)
        i_pos = span * (4 * TOK) + half * HALF + lane + (lane >> 6) * (TOK - HALF)
        first = None
        if question:
            end = jnp.int32(DOC)
            first = jnp.full((1, BLK), DOC, jnp.int32)
            for c in range(NQ - 1):
                end = end + lens[c]
                first = jnp.where(i_pos >= end, end, first)
        return dict(
            query=qd[h, half, four, 0].reshape(BLK, HD),
            grad=qd[h, half, four, 1].reshape(BLK, HD),
            i_pos=i_pos,
            first=first,
            tiles=span * 2 + 2,
            base=slot,
            span=span,
            dq=jnp.zeros((HD, BLK), F32),
            peak=None,
            total=jnp.zeros((8, BLK), F32),
            weighted=jnp.zeros((8, BLK), F32),
        )

    def score_tile(w, t):
        keys = pl.ds(t * BLK, BLK)
        score = dot_t(kb[keys, :], w["query"])
        if t >= (4 if w["first"] is not None else w["span"] * 2):
            j_pos = t * BLK + lax.broadcasted_iota(jnp.int32, (BLK, BLK), 0)
            seen = j_pos <= w["i_pos"]
            if w["first"] is not None:
                seen = seen & (j_pos >= w["first"])
            score = jnp.where(seen, score, MASKED)
        at = pl.ds((w["base"] + t) * BLK, BLK)
        s_buf[at, :] = score
        dp_buf[at, :] = dot_t(vb[keys, :], w["grad"])
        top = fold(score, jnp.max)
        w["peak"] = top if w["peak"] is None else jnp.maximum(w["peak"], top)

    def prob_tile(w, t):
        if t == 0:
            w["peak"] = jnp.max(w["peak"], axis=0, keepdims=True)
        for u in range(BLK // STRIP):
            at = pl.ds((w["base"] + t) * BLK + u * STRIP, STRIP)
            prob = jnp.exp2((s_buf[at, :] - w["peak"]) * to_log2)
            s_buf[at, :] = prob
            w["total"] = w["total"] + fold(prob, jnp.sum)
            w["weighted"] = w["weighted"] + fold(prob * dp_buf[at, :], jnp.sum)

    def grad_tile(w, t):
        if t == 0:
            w["inverse"] = 1.0 / jnp.sum(w["total"], axis=0, keepdims=True)
            w["delta"] = jnp.sum(w["weighted"], axis=0, keepdims=True) * w["inverse"]
        keys = pl.ds(t * BLK, BLK)
        low = []
        slopes = []
        for u in range(BLK // STRIP):
            at = pl.ds((w["base"] + t) * BLK + u * STRIP, STRIP)
            prob = s_buf[at, :] * w["inverse"]
            low.append(prob.astype(BF))
            slopes.append((prob * (dp_buf[at, :] - w["delta"])).astype(BF))
        score_grad = jnp.concatenate(slopes, axis=0)
        dva[keys, :] += dot_n(jnp.concatenate(low, axis=0), w["grad"])
        dka[keys, :] += dot_n(score_grad, w["query"])
        w["dq"] = w["dq"] + dot_n(kt[:, keys], score_grad)

    def give_back(h, half, w):
        span = w["span"]
        dqb[pl.ds(span * 4, 4), h, half] = (w["dq"] * scaling).T.astype(BF).reshape(4, HALF, HD)

        def give(n, carry):
            dev = span * 4 + (n + chip) % 4
            src = dqb.at[dev, h, half]
            dst = dq_out.at[pl.ds(pl.multiple_of(half * HALF, HALF), HALF), lanes(me * 2 + h)]

            @pl.when(dev == me)
            def _():
                local(src, dst, recv_dq).start()

            @pl.when(dev != me)
            def _():
                remote(src, dst, send_dq, recv_dq, dev).start()

            return carry

        lax.fori_loop(0, 4, give, 0)

    def attend(h, half, ask, doc):
        a = load(h, half, ask, 0)
        b = load(h, half, doc, ask * 2 + 2)
        for phase in (score_tile, prob_tile, grad_tile):
            for w in (b, a):
                for t in range(w["tiles"]):
                    phase(w, t)
                if phase is grad_tile:
                    give_back(h, half, w)

    acc = (dka, dva)
    outs = (dk_out, dv_out)

    def share(rb):
        for t in (0, 1):
            remote(acc[t].at[rows(rb * 2 + 1 - core)], part.at[rb, t], send_part, recv_part.at[rb], other).start()

    def close(rb):
        dev = rb * 2 + core
        local(part.at[rb], part.at[rb], recv_part.at[rb]).wait()
        for t in (0, 1):
            both = acc[t][rows(dev), :] + part[rb, t]
            if t == 0:
                both = both * scaling
            fin[rb, t] = both.astype(BF)
        for t in (0, 1):
            src = fin.at[rb, t]
            dst = outs[t].at[:, lanes(chip)]

            @pl.when(dev == me)
            def _(src=src, dst=dst, t=t):
                local(src, dst, recv_fin.at[t]).start()

            @pl.when(dev != me)
            def _(src=src, dst=dst, t=t):
                remote(src, dst, send_fin, recv_fin.at[t], dev).start()

    def chunk_step(n, carry):
        h = n // 2
        half = n % 2

        def pair_step(i, c):
            for pair in (0, 1):

                @pl.when((chip // 2 + i) % 2 == pair)
                def _(pair=pair):
                    attend(h, half, 3 - pair, pair)

            return c

        lax.fori_loop(0, 2, pair_step, 0)
        return carry

    lax.fori_loop(0, 4, chunk_step, 0)

    def share_step(i, carry):
        share((chip + 1 + i) % 8)
        return carry

    def close_step(i, carry):
        close((chip + 1 + i) % 8)
        return carry

    lax.fori_loop(0, 8, share_step, 0)
    lax.fori_loop(0, 8, close_step, 0)

    for t, (src, _) in enumerate(kv):
        local(src.at[:, pl.ds(0, 7 * HD)], src.at[:, pl.ds(0, 7 * HD)], send_kv.at[t]).wait()
        local(src, src, relay_kv.at[t]).wait()
    for t, src in enumerate(qs):
        local(src.at[:, pl.ds(0, 30 * HD)], src.at[:, pl.ds(0, 30 * HD)], send_q.at[t]).wait()
    local(part, part, send_part).wait()
    local(dqb.at[pl.ds(0, 15)], dqb.at[pl.ds(0, 15)], send_dq).wait()
    local(fin.at[pl.ds(0, 7)], fin.at[pl.ds(0, 7)], send_fin).wait()
    local(dq_out, dq_out, recv_dq).wait()
    for t in (0, 1):
        local(outs[t], outs[t], recv_fin.at[t]).wait()


def put(dq, dk, dv, dq_out, dk_out, dv_out, sems):
    pieces = ((dq, dq_out), (dk, dk_out), (dv, dv_out))
    copies = [pltpu.make_async_copy(src, dst, sems.at[n]) for n, (src, dst) in enumerate(pieces)]
    for copy in copies:
        copy.start()
    for copy in copies:
        copy.wait()


def on_device(query_rows, key_rows, value_rows, out_grad, question_lengths):
    hbm = pl.BlockSpec(memory_space=pltpu.HBM)
    any_space = pl.BlockSpec(memory_space=pl.ANY)
    dma = pltpu.SemaphoreType.DMA
    grads = pl.pallas_call(
        kernel,
        name="exchange_attend",
        out_shape=(
            pltpu.VMEM((TOK, QH * HD), BF),
            pltpu.VMEM((TOK, KVH * HD), BF),
            pltpu.VMEM((TOK, KVH * HD), BF),
        ),
        in_specs=[pl.BlockSpec(memory_space=pltpu.SMEM)] + [hbm] * 4,
        out_specs=(any_space,) * 3,
        scratch_shapes=[
            pltpu.VMEM((2, 2, DEVS, 2, HALF, HD), BF),
            pltpu.VMEM((SEQ, HD), BF),
            pltpu.VMEM((SEQ, HD), BF),
            pltpu.VMEM((HD, SEQ), BF),
            pltpu.VMEM((10 * BLK, BLK), F32),
            pltpu.VMEM((10 * BLK, BLK), F32),
            pltpu.VMEM((SEQ, HD), F32),
            pltpu.VMEM((SEQ, HD), F32),
            pltpu.VMEM((DEVS, 2, 2, HALF, HD), BF),
            pltpu.VMEM((8, 2, TOK, HD), F32),
            pltpu.VMEM((8, 2, TOK, HD), BF),
            dma((2,)),
            dma((2, DEVS)),
            dma((2,)),
            dma((2,)),
            dma((2, 2, 4)),
            dma,
            dma,
            dma,
            dma((8,)),
            dma,
            dma((2,)),
        ],
        compiler_params=pltpu.CompilerParams(
            collective_id=0, has_side_effects=True, vmem_limit_bytes=60 * 1024 * 1024
        ),
    )(question_lengths, query_rows, key_rows, value_rows, out_grad)
    return pl.pallas_call(
        put,
        name="put",
        out_shape=(
            jax.ShapeDtypeStruct((TOK, QH * HD), BF),
            jax.ShapeDtypeStruct((TOK, KVH * HD), BF),
            jax.ShapeDtypeStruct((TOK, KVH * HD), BF),
        ),
        in_specs=[any_space] * 3,
        out_specs=(any_space,) * 3,
        scratch_shapes=[dma((3,))],
    )(*(pltpu.with_memory_space_constraint(g, pltpu.VMEM) for g in grads))


def solution(mesh):
    spec = P(("grp", "sp"), None)
    return jax.shard_map(
        on_device,
        mesh=mesh,
        in_specs=(spec, spec, spec, spec, P("grp")),
        out_specs=(spec, spec, spec),
        check_vma=False,
    )
```

```python
import functools
import math

import jax
import jax.numpy as jnp
from jax import lax
from jax.experimental import pallas as pl
from jax.experimental.pallas import tpu as pltpu
from jax.sharding import PartitionSpec as P

HD = 128
QH = 32
KVH = 8
SEQ = 2048
DOC = 1024
NQ = 8
TOK = 128
HALF = 64
BLK = 256
DEVS = 16
SPANS = ((3, 2), (1, 0))
STRIP = 64
MASKED = -1e30
MESH = pl.DeviceIdType.MESH
BF = jnp.bfloat16
F32 = jnp.float32

PARTNERS = tuple(
    (a, b, c)
    for c in (0, 1)
    for a, b in ((0, 0), (0, 1), (1, 0), (0, 3), (1, 2), (0, 2), (1, 1), (1, 3))
    if (a, b, c) != (0, 0, 0)
)


def dot_t(a, b):
    return lax.dot_general(a, b, (((1,), (1,)), ((), ())), preferred_element_type=F32)


def dot_n(a, b):
    return lax.dot_general(a, b, (((1,), (0,)), ((), ())), preferred_element_type=F32)


def fold(x, op):
    return op(x.reshape(x.shape[0] // 8, 8, x.shape[1]), axis=0)


def kernel(
    lens,
    q_in,
    k_in,
    v_in,
    do_in,
    dq_out,
    dk_out,
    dv_out,
    q_own,
    k_own,
    v_own,
    do_own,
    qd,
    kb,
    vb,
    kt,
    s_buf,
    dp_buf,
    dka,
    dva,
    dqb,
    part,
    fin,
    send_kv,
    recv_kv,
    relay_kv,
    send_q,
    recv_q,
    send_dq,
    recv_dq,
    send_part,
    recv_part,
    send_fin,
    recv_fin,
    staged,
):
    grp = lax.axis_index("grp")
    me = lax.axis_index("sp")
    far = me // 8
    yy = (me // 2) % 4
    core = me % 2
    chip = me // 2
    other = chip * 2 + 1 - core
    scaling = 1.0 / math.sqrt(HD)
    to_log2 = scaling * math.log2(math.e)

    def partner(step):
        a, b, c = step
        return ((far + a) % 2) * 8 + ((yy + b) % 4) * 2 + (core + c) % 2

    def lanes(index, width=HD):
        return pl.ds(pl.multiple_of(index * width, width), width)

    def rows(index, width=TOK):
        return pl.ds(pl.multiple_of(index * width, width), width)

    def remote(src, dst, ss, rs, dev):
        return pltpu.make_async_remote_copy(
            src_ref=src, dst_ref=dst, send_sem=ss, recv_sem=rs, device_id=(grp, dev), device_id_type=MESH
        )

    def local(src, dst, sem):
        return pltpu.make_async_copy(src, dst, sem)

    staging = [
        local(src, dst, staged.at[n])
        for n, (src, dst) in enumerate(((k_in, k_own), (v_in, v_own), (q_in, q_own), (do_in, do_own)))
    ]
    for copy in staging:
        copy.start()
    barrier = pltpu.get_barrier_semaphore()
    for step in PARTNERS:
        pl.semaphore_signal(barrier, inc=1, device_id=(grp, partner(step)), device_id_type=MESH)
    dka[...] = jnp.zeros_like(dka)
    dva[...] = jnp.zeros_like(dva)
    for copy in staging:
        copy.wait()
    pl.semaphore_wait(barrier, len(PARTNERS))

    kv = ((k_own, kb), (v_own, vb))
    qs = (q_own, do_own)

    for step in PARTNERS:
        if step[2] == 0:
            dev = partner(step)
            for t, (src, dst) in enumerate(kv):
                remote(src.at[:, lanes(dev // 2)], dst.at[rows(me)], send_kv.at[t], recv_kv.at[t, me], dev).start()
    for t, (src, dst) in enumerate(kv):
        local(src.at[:, lanes(chip)], dst.at[rows(me)], recv_kv.at[t, me]).start()
        remote(src.at[:, lanes(chip)], dst.at[rows(me)], relay_kv.at[t], recv_kv.at[t, me], other).start()
    for h in (0, 1):
        for half in (0, 1):
            top = pl.ds(half * HALF, HALF)
            for step in PARTNERS:
                dev = partner(step)
                for t, src in enumerate(qs):
                    remote(
                        src.at[top, lanes(dev * 2 + h)],
                        qd.at[h, half, me, t],
                        send_q.at[t],
                        recv_q.at[h, half, me // 4],
                        dev,
                    ).start()
            for t, src in enumerate(qs):
                local(src.at[top, lanes(me * 2 + h)], qd.at[h, half, me, t], recv_q.at[h, half, me // 4]).start()

    def take(dev, pass_on):
        for t, (_, dst) in enumerate(kv):
            remote(dst.at[rows(dev)], dst.at[rows(dev)], relay_kv.at[t], recv_kv.at[t, dev], other).wait_recv()
        if pass_on:

            @pl.when(dev != me)
            def _():
                for t, (_, dst) in enumerate(kv):
                    remote(dst.at[rows(dev)], dst.at[rows(dev)], relay_kv.at[t], recv_kv.at[t, dev], other).start()

        kt[:, lanes(dev)] = kb[rows(dev), :].T

    def from_far(i, carry):
        take(((chip + 7 - i) % 8) * 2 + core, True)
        return carry

    def from_other(i, carry):
        take(((chip + 7 - i) % 8) * 2 + 1 - core, False)
        return carry

    lax.fori_loop(0, 8, from_far, 0)
    lax.fori_loop(0, 8, from_other, 0)

    def load(h, half, span, slot):
        four = pl.ds(span * 4, 4)
        local(qd.at[h, half, four], qd.at[h, half, four], recv_q.at[h, half, span]).wait()
        question = span >= 2
        lane = lax.broadcasted_iota(jnp.int32, (1, BLK), 1)
        i_pos = span * (4 * TOK) + half * HALF + lane + (lane >> 6) * (TOK - HALF)
        first = None
        if question:
            end = jnp.int32(DOC)
            first = jnp.full((1, BLK), DOC, jnp.int32)
            for c in range(NQ - 1):
                end = end + lens[c]
                first = jnp.where(i_pos >= end, end, first)
        return dict(
            query=qd[h, half, four, 0].reshape(BLK, HD),
            grad=qd[h, half, four, 1].reshape(BLK, HD),
            i_pos=i_pos,
            first=first,
            tiles=span * 2 + 2,
            base=slot,
            span=span,
            dq=jnp.zeros((HD, BLK), F32),
            peak=None,
            total=jnp.zeros((8, BLK), F32),
            weighted=jnp.zeros((8, BLK), F32),
        )

    def score_tile(w, t):
        keys = pl.ds(t * BLK, BLK)
        score = dot_t(kb[keys, :], w["query"])
        if t >= (4 if w["first"] is not None else w["span"] * 2):
            j_pos = t * BLK + lax.broadcasted_iota(jnp.int32, (BLK, BLK), 0)
            seen = j_pos <= w["i_pos"]
            if w["first"] is not None:
                seen = seen & (j_pos >= w["first"])
            score = jnp.where(seen, score, MASKED)
        at = pl.ds((w["base"] + t) * BLK, BLK)
        s_buf[at, :] = score
        dp_buf[at, :] = dot_t(vb[keys, :], w["grad"])
        top = fold(score, jnp.max)
        w["peak"] = top if w["peak"] is None else jnp.maximum(w["peak"], top)

    def prob_tile(w, t):
        if t == 0:
            w["peak"] = jnp.max(w["peak"], axis=0, keepdims=True)
        for u in range(BLK // STRIP):
            at = pl.ds((w["base"] + t) * BLK + u * STRIP, STRIP)
            prob = jnp.exp2((s_buf[at, :] - w["peak"]) * to_log2)
            s_buf[at, :] = prob
            w["total"] = w["total"] + fold(prob, jnp.sum)
            w["weighted"] = w["weighted"] + fold(prob * dp_buf[at, :], jnp.sum)

    def grad_tile(w, t):
        if t == 0:
            w["inverse"] = 1.0 / jnp.sum(w["total"], axis=0, keepdims=True)
            w["delta"] = jnp.sum(w["weighted"], axis=0, keepdims=True) * w["inverse"]
        keys = pl.ds(t * BLK, BLK)
        low = []
        slopes = []
        for u in range(BLK // STRIP):
            at = pl.ds((w["base"] + t) * BLK + u * STRIP, STRIP)
            prob = s_buf[at, :] * w["inverse"]
            low.append(prob.astype(BF))
            slopes.append((prob * (dp_buf[at, :] - w["delta"])).astype(BF))
        score_grad = jnp.concatenate(slopes, axis=0)
        dva[keys, :] += dot_n(jnp.concatenate(low, axis=0), w["grad"])
        dka[keys, :] += dot_n(score_grad, w["query"])
        w["dq"] = w["dq"] + dot_n(kt[:, keys], score_grad)

    def give_back(h, half, w):
        span = w["span"]
        dqb[pl.ds(span * 4, 4), h, half] = (w["dq"] * scaling).T.astype(BF).reshape(4, HALF, HD)

        def give(n, carry):
            dev = span * 4 + (n + chip) % 4
            src = dqb.at[dev, h, half]
            dst = dq_out.at[pl.ds(pl.multiple_of(half * HALF, HALF), HALF), lanes(me * 2 + h)]

            @pl.when(dev == me)
            def _():
                local(src, dst, recv_dq).start()

            @pl.when(dev != me)
            def _():
                remote(src, dst, send_dq, recv_dq, dev).start()

            return carry

        lax.fori_loop(0, 4, give, 0)

    def attend(h, half, later, earlier):
        a = load(h, half, later, 0)
        b = load(h, half, earlier, later * 2 + 2)
        for phase in (score_tile, prob_tile, grad_tile):
            for w in (b, a):
                for t in range(w["tiles"]):
                    phase(w, t)
                if phase is grad_tile:
                    give_back(h, half, w)

    acc = (dka, dva)
    outs = (dk_out, dv_out)

    def share(rb):
        for t in (0, 1):
            remote(acc[t].at[rows(rb * 2 + 1 - core)], part.at[rb, t], send_part, recv_part.at[rb], other).start()

    def close(rb):
        dev = rb * 2 + core
        local(part.at[rb], part.at[rb], recv_part.at[rb]).wait()
        for t in (0, 1):
            both = acc[t][rows(dev), :] + part[rb, t]
            if t == 0:
                both = both * scaling
            fin[rb, t] = both.astype(BF)
        for t in (0, 1):
            src = fin.at[rb, t]
            dst = outs[t].at[:, lanes(chip)]

            @pl.when(dev == me)
            def _(src=src, dst=dst, t=t):
                local(src, dst, recv_fin.at[t]).start()

            @pl.when(dev != me)
            def _(src=src, dst=dst, t=t):
                remote(src, dst, send_fin, recv_fin.at[t], dev).start()

    def chunk_step(n, carry):
        h = n // 2
        half = n % 2

        def pair_step(i, c):
            for pair in (0, 1):

                @pl.when((chip // 2 + i) % 2 == pair)
                def _(pair=pair):
                    attend(h, half, *SPANS[pair])

            return c

        lax.fori_loop(0, 2, pair_step, 0)
        return carry

    lax.fori_loop(0, 4, chunk_step, 0)

    def share_step(i, carry):
        share((chip + 1 + i) % 8)
        return carry

    def close_step(i, carry):
        close((chip + 1 + i) % 8)
        return carry

    lax.fori_loop(0, 8, share_step, 0)
    lax.fori_loop(0, 8, close_step, 0)

    for t, (src, _) in enumerate(kv):
        local(src.at[:, pl.ds(0, 7 * HD)], src.at[:, pl.ds(0, 7 * HD)], send_kv.at[t]).wait()
        local(src, src, relay_kv.at[t]).wait()
    for t, src in enumerate(qs):
        local(src.at[:, pl.ds(0, 30 * HD)], src.at[:, pl.ds(0, 30 * HD)], send_q.at[t]).wait()
    local(part, part, send_part).wait()
    local(dqb.at[pl.ds(0, 15)], dqb.at[pl.ds(0, 15)], send_dq).wait()
    local(fin.at[pl.ds(0, 7)], fin.at[pl.ds(0, 7)], send_fin).wait()
    local(dq_out, dq_out, recv_dq).wait()
    for t in (0, 1):
        local(outs[t], outs[t], recv_fin.at[t]).wait()


def put(dq, dk, dv, dq_out, dk_out, dv_out, sems):
    pieces = ((dq, dq_out), (dk, dk_out), (dv, dv_out))
    copies = [pltpu.make_async_copy(src, dst, sems.at[n]) for n, (src, dst) in enumerate(pieces)]
    for copy in copies:
        copy.start()
    for copy in copies:
        copy.wait()


def on_device(query_rows, key_rows, value_rows, out_grad, question_lengths):
    hbm = pl.BlockSpec(memory_space=pltpu.HBM)
    any_space = pl.BlockSpec(memory_space=pl.ANY)
    dma = pltpu.SemaphoreType.DMA
    grads = pl.pallas_call(
        kernel,
        name="exchange_attend",
        out_shape=(
            pltpu.VMEM((TOK, QH * HD), BF),
            pltpu.VMEM((TOK, KVH * HD), BF),
            pltpu.VMEM((TOK, KVH * HD), BF),
        ),
        in_specs=[pl.BlockSpec(memory_space=pltpu.SMEM)] + [hbm] * 4,
        out_specs=(any_space,) * 3,
        scratch_shapes=[
            pltpu.VMEM((TOK, QH * HD), BF),
            pltpu.VMEM((TOK, KVH * HD), BF),
            pltpu.VMEM((TOK, KVH * HD), BF),
            pltpu.VMEM((TOK, QH * HD), BF),
            pltpu.VMEM((2, 2, DEVS, 2, HALF, HD), BF),
            pltpu.VMEM((SEQ, HD), BF),
            pltpu.VMEM((SEQ, HD), BF),
            pltpu.VMEM((HD, SEQ), BF),
            pltpu.VMEM((14 * BLK, BLK), F32),
            pltpu.VMEM((14 * BLK, BLK), F32),
            pltpu.VMEM((SEQ, HD), F32),
            pltpu.VMEM((SEQ, HD), F32),
            pltpu.VMEM((DEVS, 2, 2, HALF, HD), BF),
            pltpu.VMEM((8, 2, TOK, HD), F32),
            pltpu.VMEM((8, 2, TOK, HD), BF),
            dma((2,)),
            dma((2, DEVS)),
            dma((2,)),
            dma((2,)),
            dma((2, 2, 4)),
            dma,
            dma,
            dma,
            dma((8,)),
            dma,
            dma((2,)),
            dma((4,)),
        ],
        compiler_params=pltpu.CompilerParams(
            collective_id=0, has_side_effects=True, vmem_limit_bytes=60 * 1024 * 1024
        ),
    )(question_lengths, query_rows, key_rows, value_rows, out_grad)
    return pl.pallas_call(
        put,
        name="put",
        out_shape=(
            jax.ShapeDtypeStruct((TOK, QH * HD), BF),
            jax.ShapeDtypeStruct((TOK, KVH * HD), BF),
            jax.ShapeDtypeStruct((TOK, KVH * HD), BF),
        ),
        in_specs=[any_space] * 3,
        out_specs=(any_space,) * 3,
        scratch_shapes=[dma((3,))],
    )(*(pltpu.with_memory_space_constraint(g, pltpu.VMEM) for g in grads))


def solution(mesh):
    spec = P(("grp", "sp"), None)
    return jax.shard_map(
        on_device,
        mesh=mesh,
        in_specs=(spec, spec, spec, spec, P("grp")),
        out_specs=(spec, spec, spec),
        check_vma=False,
    )
```

```python
import functools
import math

import jax
import jax.numpy as jnp
from jax import lax
from jax.experimental import pallas as pl
from jax.experimental.pallas import tpu as pltpu
from jax.sharding import PartitionSpec as P

HD = 128
QH = 32
KVH = 8
SEQ = 2048
DOC = 1024
NQ = 8
TOK = 128
HALF = 64
BLK = 256
DEVS = 16
SPANS = ((3, 2), (1, 0))
STRIP = 64
MASKED = -1e30
MESH = pl.DeviceIdType.MESH
BF = jnp.bfloat16
F32 = jnp.float32

PARTNERS = tuple(
    (a, b, c)
    for c in (0, 1)
    for a, b in ((0, 0), (0, 1), (1, 0), (0, 3), (1, 2), (0, 2), (1, 1), (1, 3))
    if (a, b, c) != (0, 0, 0)
)


def dot_t(a, b):
    return lax.dot_general(a, b, (((1,), (1,)), ((), ())), preferred_element_type=F32)


def dot_n(a, b):
    return lax.dot_general(a, b, (((1,), (0,)), ((), ())), preferred_element_type=F32)


def fold(x, op):
    return op(x.reshape(x.shape[0] // 8, 8, x.shape[1]), axis=0)


def kernel(
    lens,
    q_in,
    k_in,
    v_in,
    do_in,
    dq_out,
    dk_out,
    dv_out,
    q_own,
    k_own,
    v_own,
    do_own,
    qd,
    kb,
    vb,
    kt,
    s_buf,
    dp_buf,
    dka,
    dva,
    dqb,
    part,
    fin,
    send_kv,
    recv_kv,
    relay_kv,
    send_q,
    recv_q,
    send_dq,
    recv_dq,
    send_part,
    recv_part,
    send_fin,
    recv_fin,
    staged,
):
    grp = lax.axis_index("grp")
    me = lax.axis_index("sp")
    far = me // 8
    yy = (me // 2) % 4
    core = me % 2
    chip = me // 2
    other = chip * 2 + 1 - core
    scaling = 1.0 / math.sqrt(HD)
    to_log2 = scaling * math.log2(math.e)

    def partner(step):
        a, b, c = step
        return ((far + a) % 2) * 8 + ((yy + b) % 4) * 2 + (core + c) % 2

    def lanes(index, width=HD):
        return pl.ds(pl.multiple_of(index * width, width), width)

    def rows(index, width=TOK):
        return pl.ds(pl.multiple_of(index * width, width), width)

    def remote(src, dst, ss, rs, dev):
        return pltpu.make_async_remote_copy(
            src_ref=src, dst_ref=dst, send_sem=ss, recv_sem=rs, device_id=(grp, dev), device_id_type=MESH
        )

    def local(src, dst, sem):
        return pltpu.make_async_copy(src, dst, sem)

    staging = [
        local(src, dst, staged.at[n])
        for n, (src, dst) in enumerate(((k_in, k_own), (v_in, v_own), (q_in, q_own), (do_in, do_own)))
    ]
    for copy in staging:
        copy.start()
    barrier = pltpu.get_barrier_semaphore()
    for step in PARTNERS:
        pl.semaphore_signal(barrier, inc=1, device_id=(grp, partner(step)), device_id_type=MESH)
    dka[...] = jnp.zeros_like(dka)
    dva[...] = jnp.zeros_like(dva)
    for copy in staging:
        copy.wait()
    pl.semaphore_wait(barrier, len(PARTNERS))

    kv = ((k_own, kb), (v_own, vb))
    qs = (q_own, do_own)

    for step in PARTNERS:
        if step[2] == 0:
            dev = partner(step)
            for t, (src, dst) in enumerate(kv):
                remote(src.at[:, lanes(dev // 2)], dst.at[rows(me)], send_kv.at[t], recv_kv.at[t, me], dev).start()
    for t, (src, dst) in enumerate(kv):
        local(src.at[:, lanes(chip)], dst.at[rows(me)], recv_kv.at[t, me]).start()
        remote(src.at[:, lanes(chip)], dst.at[rows(me)], relay_kv.at[t], recv_kv.at[t, me], other).start()
    for h in (0, 1):
        for half in (0, 1):
            top = pl.ds(half * HALF, HALF)
            for step in PARTNERS:
                dev = partner(step)
                for t, src in enumerate(qs):
                    remote(
                        src.at[top, lanes(dev * 2 + h)],
                        qd.at[h, half, me, t],
                        send_q.at[t],
                        recv_q.at[h, half, me // 4],
                        dev,
                    ).start()
            for t, src in enumerate(qs):
                local(src.at[top, lanes(me * 2 + h)], qd.at[h, half, me, t], recv_q.at[h, half, me // 4]).start()

    def take(dev, pass_on):
        for t, (_, dst) in enumerate(kv):
            remote(dst.at[rows(dev)], dst.at[rows(dev)], relay_kv.at[t], recv_kv.at[t, dev], other).wait_recv()
        if pass_on:

            @pl.when(dev != me)
            def _():
                for t, (_, dst) in enumerate(kv):
                    remote(dst.at[rows(dev)], dst.at[rows(dev)], relay_kv.at[t], recv_kv.at[t, dev], other).start()

        kt[:, lanes(dev)] = kb[rows(dev), :].T

    def from_far(i, carry):
        take(((chip + 7 - i) % 8) * 2 + core, True)
        return carry

    def from_other(i, carry):
        take(((chip + 7 - i) % 8) * 2 + 1 - core, False)
        return carry

    lax.fori_loop(0, 8, from_far, 0)
    lax.fori_loop(0, 8, from_other, 0)

    def load(h, half, span, slot):
        four = pl.ds(span * 4, 4)
        local(qd.at[h, half, four], qd.at[h, half, four], recv_q.at[h, half, span]).wait()
        question = span >= 2
        lane = lax.broadcasted_iota(jnp.int32, (1, BLK), 1)
        i_pos = span * (4 * TOK) + half * HALF + lane + (lane >> 6) * (TOK - HALF)
        first = None
        if question:
            end = jnp.int32(DOC)
            first = jnp.full((1, BLK), DOC, jnp.int32)
            for c in range(NQ - 1):
                end = end + lens[c]
                first = jnp.where(i_pos >= end, end, first)
        return dict(
            query=qd[h, half, four, 0].reshape(BLK, HD),
            grad=qd[h, half, four, 1].reshape(BLK, HD),
            i_pos=i_pos,
            first=first,
            tiles=span * 2 + 2,
            base=slot,
            span=span,
            dq=jnp.zeros((HD, BLK), F32),
            peak=None,
            total=jnp.zeros((8, BLK), F32),
            weighted=jnp.zeros((8, BLK), F32),
        )

    def score_tile(w, t):
        keys = pl.ds(t * BLK, BLK)
        score = dot_t(kb[keys, :], w["query"])
        if t >= (4 if w["first"] is not None else w["span"] * 2):
            j_pos = t * BLK + lax.broadcasted_iota(jnp.int32, (BLK, BLK), 0)
            seen = j_pos <= w["i_pos"]
            if w["first"] is not None:
                seen = seen & (j_pos >= w["first"])
            score = jnp.where(seen, score, MASKED)
        at = pl.ds((w["base"] + t) * BLK, BLK)
        s_buf[at, :] = score
        dp_buf[at, :] = dot_t(vb[keys, :], w["grad"])
        top = fold(score, jnp.max)
        w["peak"] = top if w["peak"] is None else jnp.maximum(w["peak"], top)

    def prob_tile(w, t):
        if t == 0:
            w["peak"] = jnp.max(w["peak"], axis=0, keepdims=True)
        for u in range(BLK // STRIP):
            at = pl.ds((w["base"] + t) * BLK + u * STRIP, STRIP)
            prob = jnp.exp2((s_buf[at, :] - w["peak"]) * to_log2)
            s_buf[at, :] = prob
            w["total"] = w["total"] + fold(prob, jnp.sum)
            w["weighted"] = w["weighted"] + fold(prob * dp_buf[at, :], jnp.sum)

    def grad_tile(w, t):
        if t == 0:
            w["inverse"] = 1.0 / jnp.sum(w["total"], axis=0, keepdims=True)
            w["delta"] = jnp.sum(w["weighted"], axis=0, keepdims=True) * w["inverse"]
        keys = pl.ds(t * BLK, BLK)
        low = []
        slopes = []
        for u in range(BLK // STRIP):
            at = pl.ds((w["base"] + t) * BLK + u * STRIP, STRIP)
            prob = s_buf[at, :] * w["inverse"]
            low.append(prob.astype(BF))
            slopes.append((prob * (dp_buf[at, :] - w["delta"])).astype(BF))
        score_grad = jnp.concatenate(slopes, axis=0)
        dva[keys, :] += dot_n(jnp.concatenate(low, axis=0), w["grad"])
        dka[keys, :] += dot_n(score_grad, w["query"])
        w["dq"] = w["dq"] + dot_n(kt[:, keys], score_grad)

    def give_back(h, half, w):
        span = w["span"]
        dqb[pl.ds(span * 4, 4), h, half] = (w["dq"] * scaling).T.astype(BF).reshape(4, HALF, HD)

        def give(n, carry):
            dev = span * 4 + (n + chip) % 4
            src = dqb.at[dev, h, half]
            dst = dq_out.at[pl.ds(pl.multiple_of(half * HALF, HALF), HALF), lanes(me * 2 + h)]

            @pl.when(dev == me)
            def _():
                local(src, dst, recv_dq).start()

            @pl.when(dev != me)
            def _():
                remote(src, dst, send_dq, recv_dq, dev).start()

            return carry

        lax.fori_loop(0, 4, give, 0)

    def attend(h, half, later, earlier):
        a = load(h, half, later, 0)
        b = load(h, half, earlier, later * 2 + 2)
        for phase in (score_tile, prob_tile, grad_tile):
            for w in (b, a):
                for t in range(w["tiles"]):
                    phase(w, t)
        for w in (b, a):
            give_back(h, half, w)

    acc = (dka, dva)
    outs = (dk_out, dv_out)

    def share(rb):
        for t in (0, 1):
            remote(acc[t].at[rows(rb * 2 + 1 - core)], part.at[rb, t], send_part, recv_part.at[rb], other).start()

    def close(rb):
        dev = rb * 2 + core
        local(part.at[rb], part.at[rb], recv_part.at[rb]).wait()
        for t in (0, 1):
            both = acc[t][rows(dev), :] + part[rb, t]
            if t == 0:
                both = both * scaling
            fin[rb, t] = both.astype(BF)
        for t in (0, 1):
            src = fin.at[rb, t]
            dst = outs[t].at[:, lanes(chip)]

            @pl.when(dev == me)
            def _(src=src, dst=dst, t=t):
                local(src, dst, recv_fin.at[t]).start()

            @pl.when(dev != me)
            def _(src=src, dst=dst, t=t):
                remote(src, dst, send_fin, recv_fin.at[t], dev).start()

    def chunk_step(n, carry):
        h = n // 2
        half = n % 2

        def pair_step(i, c):
            for pair in (0, 1):

                @pl.when((chip // 2 + i) % 2 == pair)
                def _(pair=pair):
                    attend(h, half, *SPANS[pair])

            return c

        lax.fori_loop(0, 2, pair_step, 0)
        return carry

    lax.fori_loop(0, 4, chunk_step, 0)

    def share_step(i, carry):
        share((chip + 1 + i) % 8)
        return carry

    def close_step(i, carry):
        close((chip + 1 + i) % 8)
        return carry

    lax.fori_loop(0, 8, share_step, 0)
    lax.fori_loop(0, 8, close_step, 0)

    for t, (src, _) in enumerate(kv):
        local(src.at[:, pl.ds(0, 7 * HD)], src.at[:, pl.ds(0, 7 * HD)], send_kv.at[t]).wait()
        local(src, src, relay_kv.at[t]).wait()
    for t, src in enumerate(qs):
        local(src.at[:, pl.ds(0, 30 * HD)], src.at[:, pl.ds(0, 30 * HD)], send_q.at[t]).wait()
    local(part, part, send_part).wait()
    local(dqb.at[pl.ds(0, 15)], dqb.at[pl.ds(0, 15)], send_dq).wait()
    local(fin.at[pl.ds(0, 7)], fin.at[pl.ds(0, 7)], send_fin).wait()
    local(dq_out, dq_out, recv_dq).wait()
    for t in (0, 1):
        local(outs[t], outs[t], recv_fin.at[t]).wait()


def put(dq, dk, dv, dq_out, dk_out, dv_out, sems):
    pieces = ((dq, dq_out), (dk, dk_out), (dv, dv_out))
    copies = [pltpu.make_async_copy(src, dst, sems.at[n]) for n, (src, dst) in enumerate(pieces)]
    for copy in copies:
        copy.start()
    for copy in copies:
        copy.wait()


def on_device(query_rows, key_rows, value_rows, out_grad, question_lengths):
    hbm = pl.BlockSpec(memory_space=pltpu.HBM)
    any_space = pl.BlockSpec(memory_space=pl.ANY)
    dma = pltpu.SemaphoreType.DMA
    grads = pl.pallas_call(
        kernel,
        name="exchange_attend",
        out_shape=(
            pltpu.VMEM((TOK, QH * HD), BF),
            pltpu.VMEM((TOK, KVH * HD), BF),
            pltpu.VMEM((TOK, KVH * HD), BF),
        ),
        in_specs=[pl.BlockSpec(memory_space=pltpu.SMEM)] + [hbm] * 4,
        out_specs=(any_space,) * 3,
        scratch_shapes=[
            pltpu.VMEM((TOK, QH * HD), BF),
            pltpu.VMEM((TOK, KVH * HD), BF),
            pltpu.VMEM((TOK, KVH * HD), BF),
            pltpu.VMEM((TOK, QH * HD), BF),
            pltpu.VMEM((2, 2, DEVS, 2, HALF, HD), BF),
            pltpu.VMEM((SEQ, HD), BF),
            pltpu.VMEM((SEQ, HD), BF),
            pltpu.VMEM((HD, SEQ), BF),
            pltpu.VMEM((14 * BLK, BLK), F32),
            pltpu.VMEM((14 * BLK, BLK), F32),
            pltpu.VMEM((SEQ, HD), F32),
            pltpu.VMEM((SEQ, HD), F32),
            pltpu.VMEM((DEVS, 2, 2, HALF, HD), BF),
            pltpu.VMEM((8, 2, TOK, HD), F32),
            pltpu.VMEM((8, 2, TOK, HD), BF),
            dma((2,)),
            dma((2, DEVS)),
            dma((2,)),
            dma((2,)),
            dma((2, 2, 4)),
            dma,
            dma,
            dma,
            dma((8,)),
            dma,
            dma((2,)),
            dma((4,)),
        ],
        compiler_params=pltpu.CompilerParams(
            collective_id=0, has_side_effects=True, vmem_limit_bytes=60 * 1024 * 1024
        ),
    )(question_lengths, query_rows, key_rows, value_rows, out_grad)
    return pl.pallas_call(
        put,
        name="put",
        out_shape=(
            jax.ShapeDtypeStruct((TOK, QH * HD), BF),
            jax.ShapeDtypeStruct((TOK, KVH * HD), BF),
            jax.ShapeDtypeStruct((TOK, KVH * HD), BF),
        ),
        in_specs=[any_space] * 3,
        out_specs=(any_space,) * 3,
        scratch_shapes=[dma((3,))],
    )(*(pltpu.with_memory_space_constraint(g, pltpu.VMEM) for g in grads))


def solution(mesh):
    spec = P(("grp", "sp"), None)
    return jax.shard_map(
        on_device,
        mesh=mesh,
        in_specs=(spec, spec, spec, spec, P("grp")),
        out_specs=(spec, spec, spec),
        check_vma=False,
    )
```
